16 devices in a mesh: rep: 1, dp: 16 (over x, y, z, core).
Axes of the slice: x: 2, y: 2, z: 2, core: 2. Of those that a mesh axis runs over, the one named last changes fastest.
Arguments:
- x: bfloat16 [16, 2048, 1024], P(('rep', 'dp'))
- dy: bfloat16 [16, 2048, 1024], P(('rep', 'dp'))
- wq: bfloat16 [2, 1024, 1024], P(None, 'dp')
- wk: bfloat16 [2, 1024, 1024], P(None, 'dp')
- wv: bfloat16 [2, 1024, 1024], P(None, 'dp')
- wo: bfloat16 [2, 1024, 1024], P(None, 'dp')
- w_gate: bfloat16 [2, 1024, 3072], P(None, 'dp')
- w_up: bfloat16 [2, 1024, 3072], P(None, 'dp')
- w_down: bfloat16 [2, 3072, 1024], P(None, 'dp')
- m_wq: float32 [2, 1024, 1024], P(None, 'dp')
- m_wk: float32 [2, 1024, 1024], P(None, 'dp')
- m_wv: float32 [2, 1024, 1024], P(None, 'dp')
- m_wo: float32 [2, 1024, 1024], P(None, 'dp')
- m_w_gate: float32 [2, 1024, 3072], P(None, 'dp')
- m_w_up: float32 [2, 1024, 3072], P(None, 'dp')
- m_w_down: float32 [2, 3072, 1024], P(None, 'dp')
- v_wq: float32 [2, 1024, 1024], P(None, 'dp')
- v_wk: float32 [2, 1024, 1024], P(None, 'dp')
- v_wv: float32 [2, 1024, 1024], P(None, 'dp')
- v_wo: float32 [2, 1024, 1024], P(None, 'dp')
- v_w_gate: float32 [2, 1024, 3072], P(None, 'dp')
- v_w_up: float32 [2, 1024, 3072], P(None, 'dp')
- v_w_down: float32 [2, 3072, 1024], P(None, 'dp')
Outputs:
- output 1: bfloat16 [2, 1024, 1024], P('rep', 'dp')
- output 2: bfloat16 [2, 1024, 1024], P('rep', 'dp')
- output 3: bfloat16 [2, 1024, 1024], P('rep', 'dp')
- output 4: bfloat16 [2, 1024, 1024], P('rep', 'dp')
- output 5: bfloat16 [2, 1024, 3072], P('rep', 'dp')
- output 6: bfloat16 [2, 1024, 3072], P('rep', 'dp')
- output 7: bfloat16 [2, 3072, 1024], P('rep', 'dp')
- output 8: float32 [2, 1024, 1024], P('rep', 'dp')
- output 9: float32 [2, 1024, 1024], P('rep', 'dp')
- output 10: float32 [2, 1024, 1024], P('rep', 'dp')
- output 11: float32 [2, 1024, 1024], P('rep', 'dp')
- output 12: float32 [2, 1024, 3072], P('rep', 'dp')
- output 13: float32 [2, 1024, 3072], P('rep', 'dp')
- output 14: float32 [2, 3072, 1024], P('rep', 'dp')
- output 15: float32 [2, 1024, 1024], P('rep', 'dp')
- output 16: float32 [2, 1024, 1024], P('rep', 'dp')
- output 17: float32 [2, 1024, 1024], P('rep', 'dp')
- output 18: float32 [2, 1024, 1024], P('rep', 'dp')
- output 19: float32 [2, 1024, 3072], P('rep', 'dp')
- output 20: float32 [2, 1024, 3072], P('rep', 'dp')
- output 21: float32 [2, 3072, 1024], P('rep', 'dp')
All inputs are finite; a program needn't handle non-finite values.
Results may differ from the reference program's by a relative error of at most 0.024.
Values are sent between devices in bfloat16 or wider.
A program may use at most 2 GiB of HBM per device.

```python
import jax
import jax.numpy as jnp
from jax import lax

SEQUENCES = 16
TOKENS = 2048
D = 1024
HEADS = 8
KV_HEADS = 8
HEAD = 128
FF = 3072
LAYERS = 2
THETA = 10000
NAMES = ("wq", "wk", "wv", "wo", "w_gate", "w_up", "w_down")
SHAPES = {
    "wq": (LAYERS, D, HEADS * HEAD),
    "wk": (LAYERS, D, KV_HEADS * HEAD),
    "wv": (LAYERS, D, KV_HEADS * HEAD),
    "wo": (LAYERS, HEADS * HEAD, D),
    "w_gate": (LAYERS, D, FF),
    "w_up": (LAYERS, D, FF),
    "w_down": (LAYERS, FF, D),
}


def bump(key, n, height):
    away = (jnp.arange(n, dtype=jnp.int32) - jax.random.randint(key, (), 0, n, jnp.int32)) % n
    return jnp.where(away < n // 8, height, 1.0)


def together(key, own, strength):
    shared = jax.random.normal(key, own.shape[1:], jnp.float32)
    return (own + strength * shared) * lax.rsqrt(1 + strength * strength)


def setup_inputs(seed: int = 0, part: int = 0) -> dict:
    kx, kdy, ka, kb, kz, kf, kh, kl, *keys = jax.random.split(jax.random.key(seed), 8 + 3 * len(NAMES))
    kx, kdy, ka, kb = (jax.random.fold_in(k, part) for k in (kx, kdy, ka, kb))
    kw, km, kv = (keys[i::3] for i in range(3))
    shape = (SEQUENCES, TOKENS, D)
    much_x, much_dy = jax.random.uniform(kz, (2,), jnp.float32, 0.0, 1.0)
    loud = 2.0 ** jax.random.uniform(jax.random.fold_in(kz, 1), (), jnp.float32, -1.0, 2.0)
    layers = 2.0 ** jax.random.uniform(kl, (LAYERS, 1, 1), jnp.float32, -1.0, 1.0)
    times = {"wq": 1.0, "wk": 1.0, "wv": 2.0, "wo": layers, "w_gate": 1.0, "w_up": bump(kh, FF, 4.0), "w_down": layers}
    x = together(ka, jax.random.normal(kx, shape, jnp.float32), much_x) * bump(kf, D, 4.0)
    dy = together(kb, jax.random.normal(kdy, shape, jnp.float32), much_dy)
    drawn = {"x": x.astype(jnp.bfloat16), "dy": (loud * dy * (SEQUENCES * TOKENS) ** -0.5).astype(jnp.bfloat16)}
    for key, name in zip(kw, NAMES, strict=True):
        drawn[name] = (jax.random.normal(key, SHAPES[name], jnp.float32) * SHAPES[name][1] ** -0.5 * times[name]).astype(jnp.bfloat16)
    for key, name in zip(km, NAMES, strict=True):
        drawn[f"m_{name}"] = 0.1 * jax.random.normal(key, SHAPES[name], jnp.float32)
    for key, name in zip(kv, NAMES, strict=True):
        drawn[f"v_{name}"] = jax.random.uniform(key, SHAPES[name], jnp.float32, 0.02, 0.06)
    return drawn


def matmul(a, w):
    return jnp.dot(a, w, preferred_element_type=jnp.float32).astype(jnp.bfloat16)


def normed(h):
    wide = h.astype(jnp.float32)
    scale = lax.rsqrt(jnp.mean(wide**2, -1, keepdims=True) + 1e-6)
    return (wide * scale).astype(jnp.bfloat16)


def turned(t, theta):
    half = t.shape[-1] // 2
    angle = jnp.arange(t.shape[0], dtype=jnp.float32)[:, None] * theta ** (-jnp.arange(half, dtype=jnp.float32) / half)
    cos, sin = jnp.cos(angle)[:, None], jnp.sin(angle)[:, None]
    a, b = t[..., :half].astype(jnp.float32), t[..., half:].astype(jnp.float32)
    return jnp.concatenate([a * cos - b * sin, b * cos + a * sin], -1).astype(jnp.bfloat16)


def seen_by(q, k, v):
    tokens, kv = q.shape[0], k.shape[1]
    q = q.reshape(tokens, kv, -1, q.shape[-1])
    scores = jnp.einsum("tgsd,ugd->gstu", q.astype(jnp.float32), k.astype(jnp.float32)) * q.shape[-1] ** -0.5
    place = jnp.arange(tokens)
    weights = jax.nn.softmax(jnp.where(place[:, None] >= place, scores, -jnp.inf), -1).astype(jnp.bfloat16)
    return jnp.einsum("gstu,ugd->tgsd", weights.astype(jnp.float32), v.astype(jnp.float32)).astype(jnp.bfloat16).reshape(tokens, -1)


def layer(h, w):
    a = normed(h)
    q, k = (turned(matmul(a, w[name]).reshape(h.shape[0], -1, HEAD), THETA) for name in ("wq", "wk"))
    h = h + matmul(seen_by(q, k, matmul(a, w["wv"]).reshape(h.shape[0], -1, HEAD)), w["wo"])
    b = normed(h)
    gate = jnp.dot(b, w["w_gate"], preferred_element_type=jnp.float32)
    up = jnp.dot(b, w["w_up"], preferred_element_type=jnp.float32)
    return h + matmul((jax.nn.silu(gate) * up).astype(jnp.bfloat16), w["w_down"])


def adamw(w, m, v, g):
    m = 0.9 * m + 0.1 * g
    v = 0.95 * v + 0.05 * g * g
    step = m * lax.rsqrt(v + 1e-8) + 0.1 * w
    return (w - 0.02 * step).astype(jnp.bfloat16), m, v


def clipped(gradients, sum_of_squares, count):
    factor = jnp.minimum(1.0, 0.5 * lax.rsqrt(sum_of_squares / count + 1e-30))
    return [g * factor for g in gradients]


def stack(weights, h):
    return lax.scan(lambda h, w: (layer(h, w), None), h, weights)[0]


def reference(x, dy, wq, wk, wv, wo, w_gate, w_up, w_down, m_wq, m_wk, m_wv, m_wo, m_w_gate, m_w_up, m_w_down, v_wq, v_wk, v_wv, v_wo, v_w_gate, v_w_up, v_w_down):
    weights = dict(zip(NAMES, (wq, wk, wv, wo, w_gate, w_up, w_down), strict=True))

    def take(so_far, sequence):
        h, by_y = sequence
        _, back = jax.vjp(stack, weights, h)
        by_weights, by_h = back(by_y)
        return jax.tree.map(lambda total, term: total + term.astype(jnp.float32), so_far, by_weights), by_h

    none_yet = {name: jnp.zeros(w.shape, jnp.float32) for name, w in weights.items()}
    by_weights, by_x = lax.scan(take, none_yet, (x, dy))
    gradients = [by_weights[name].astype(jnp.bfloat16).astype(jnp.float32) for name in NAMES]
    gradients = clipped(gradients, sum(jnp.sum(g * g) for g in gradients), sum(g.size for g in gradients))
    first = (m_wq, m_wk, m_wv, m_wo, m_w_gate, m_w_up, m_w_down)
    second = (v_wq, v_wk, v_wv, v_wo, v_w_gate, v_w_up, v_w_down)
    new = [adamw(weights[name].astype(jnp.float32), m, v, g) for name, m, v, g in zip(NAMES, first, second, gradients, strict=True)]
    return tuple(one[which] for which in range(3) for one in new)
```

```python
import functools

import jax
import jax.numpy as jnp
from jax import lax
from jax.experimental import pallas as pl
from jax.experimental.pallas import tpu as pltpu
from jax.sharding import PartitionSpec as P

NEG = -1e30
HIDDEN = 2 * NEG
LOG2E = 1.4426950408889634
VMEM = 60 * 2**20
HEAD = 128
THETA = 10000
NAMES = ("wq", "wk", "wv", "wo", "w_gate", "w_up", "w_down")
LOW, WIDE = jnp.bfloat16, jnp.float32


def _dot(a, b, ca, cb):
    return lax.dot_general(a, b, (((ca,), (cb,)), ((), ())), preferred_element_type=jnp.float32)


def call(body, name, grid, ins, outs, scratch=(), aliases=None, flops=0, trans=0, sem=None):
    specs = []
    for array, block, where, *buffers in ins:
        if block is None:
            specs.append(pl.BlockSpec(memory_space=pl.ANY))
        elif buffers:
            specs.append(pl.BlockSpec(block, where, pipeline_mode=pl.Buffered(buffers[0])))
        else:
            specs.append(pl.BlockSpec(block, where))
    out_specs = [pl.BlockSpec(block, where) for _, _, block, where in outs]
    shapes = [jax.ShapeDtypeStruct(shape, dtype) for shape, dtype, _, _ in outs]
    moved = sum(a.size * a.dtype.itemsize for a, *_ in ins) + sum(s.size * s.dtype.itemsize for s in shapes)
    return pl.pallas_call(
        body, name=name, grid=grid, in_specs=specs, out_specs=out_specs, out_shape=shapes, scratch_shapes=list(scratch),
        input_output_aliases=aliases or {},
        compiler_params=pltpu.CompilerParams(dimension_semantics=("arbitrary",) * len(grid), vmem_limit_bytes=VMEM),
        cost_estimate=pl.CostEstimate(flops=int(flops), transcendentals=int(trans), bytes_accessed=int(moved)),
    )(*(a for a, *_ in ins))


def flat(ref):
    w = ref[...]
    return w.reshape(w.shape[0] * w.shape[1], w.shape[2])


def rms(wide):
    return lax.rsqrt(jnp.mean(wide * wide, -1, keepdims=True) + 1e-6)


def turn(x, cos, sin):
    return x * cos + pltpu.roll(x, 64, 1) * sin


def _qkv(h_ref, wq_ref, wk_ref, wv_ref, cos_ref, sin_ref, a_ref, out_ref):
    d = h_ref.shape[1]
    wide = h_ref[...].astype(WIDE)
    a = (wide * rms(wide)).astype(LOW)
    a_ref[...] = a
    cos, sin = cos_ref[...], sin_ref[...]
    for n, w_ref in enumerate((wq_ref, wk_ref, wv_ref)):
        for at in range(0, d, 256):
            r = _dot(a, w_ref[:, :, at : at + 256].reshape(d, 256), 1, 0).astype(LOW)
            if n < 2:
                r = jnp.concatenate([turn(r[:, i : i + HEAD].astype(WIDE), cos, sin).astype(LOW) for i in (0, HEAD)], axis=1)
            out_ref[:, n * d + at : n * d + at + 256] = r


def qkv_of(h, first, cos, sin):
    t, d = h.shape
    n = first.shape[0]
    bt = 512
    rows = d // n
    ins = [(h, (bt, d), lambda i: (i, 0))]
    ins += [(first, (n, rows, d), lambda i, j=j: (0, j, 0)) for j in range(3)]
    ins += [(cos, (bt, HEAD), lambda i: (i, 0)), (sin, (bt, HEAD), lambda i: (i, 0))]
    outs = [((t, d), LOW, (bt, d), lambda i: (i, 0)), ((t, 3 * d), LOW, (bt, 3 * d), lambda i: (i, 0))]
    return call(_qkv, "qkv", (t // bt,), ins, outs, flops=6 * t * d * d)


def seen(keys, queries):
    return lax.broadcasted_iota(jnp.int32, (keys, queries), 1) >= lax.broadcasted_iota(jnp.int32, (keys, queries), 0)


def _attend(q_ref, k_ref, v_ref, o_ref, lse_ref, top_s, mix_s, *, scale):
    bq, d = q_ref.shape[0], HEAD
    heads = q_ref.shape[1] // d
    iq = pl.program_id(0)
    e = scale * LOG2E
    top_s[...] = jnp.full(top_s.shape, NEG, WIDE)
    mix_s[...] = jnp.zeros(mix_s.shape, WIDE)

    def block(start, keys, first, masked):
        here, mine = pl.ds(pl.multiple_of(start, keys), keys), slice(first, bq)
        ones = jnp.ones((8, keys), LOW)
        scores = [_dot(k_ref[here, i * d : i * d + d], q_ref[mine, i * d : i * d + d], 1, 1) for i in range(heads)]
        ok = seen(keys, bq - first) if masked else None
        weights, keeps = [], []
        for i, s in enumerate(scores):
            if masked:
                s = jnp.where(ok, s, HIDDEN)
            old = top_s[i : i + 1, mine]
            top = jnp.maximum(old, s.max(axis=0, keepdims=True))
            top_s[i : i + 1, mine] = top
            weights.append(jnp.exp2((s - top) * e).astype(LOW))
            keeps.append(jnp.exp2((old - top) * e))
        for i, (p, keep) in enumerate(zip(weights, keeps)):
            values = jnp.concatenate([v_ref[here, i * d : i * d + d].T, ones], axis=0)
            mix_s[i, :, mine] = mix_s[i, :, mine] * keep + _dot(values, p, 1, 0)

    lax.fori_loop(0, iq, lambda j, _: block(j * bq, bq, 0, False), None)
    block(iq * bq, bq // 2, 0, True)
    block(iq * bq + bq // 2, bq // 2, bq // 2, True)
    for i in range(heads):
        total = mix_s[i, d : d + 1, :]
        o_ref[:, i * d : i * d + d] = (mix_s[i, :d, :] * (1 / total)).T.astype(LOW)
        lse_ref[i // 4, i % 4 : i % 4 + 1, :] = top_s[i : i + 1, :] * scale + jnp.log(total)


def attend(qkv):
    t, d = qkv.shape[0], qkv.shape[1] // 3
    heads, bq = d // HEAD, 512
    ins = [(qkv, (bq, d), lambda i: (i, 0)), (qkv, (t, d), lambda i: (0, 1)), (qkv, (t, d), lambda i: (0, 2))]
    outs = [((t, d), LOW, (bq, d), lambda i: (i, 0)),
            ((heads // 4, 4, t), WIDE, (heads // 4, 4, bq), lambda i: (0, 0, i))]
    scratch = [pltpu.VMEM((heads, bq), WIDE), pltpu.VMEM((heads, HEAD + 8, bq), WIDE)]
    return call(functools.partial(_attend, scale=HEAD**-0.5), "attend", (t // bq,), ins, outs, scratch,
                flops=4 * t * t * d, trans=heads * t * t)


def _out(o_ref, h_ref, w_ref, h2_ref, b_ref):
    r = _dot(o_ref[...], flat(w_ref), 1, 0).astype(LOW)
    h2 = (h_ref[...].astype(WIDE) + r.astype(WIDE)).astype(LOW)
    h2_ref[...] = h2
    wide = h2.astype(WIDE)
    b_ref[...] = (wide * rms(wide)).astype(LOW)


def out_of(o, h, first):
    t, d = h.shape
    n, bt = first.shape[0], 512
    row = lambda i: (i, 0)
    ins = [(o, (bt, d), row), (h, (bt, d), row), (first, (n, d // n, d), lambda i: (0, 3, 0))]
    outs = [((t, d), LOW, (bt, d), row)] * 2
    return call(_out, "out", (t // bt,), ins, outs, flops=2 * t * d * d)


def _up(b_ref, g_ref, u_ref, gu_ref, act_ref):
    wg, wu = flat(g_ref), flat(u_ref)
    for at in range(0, b_ref.shape[0], 256):
        b = b_ref[at : at + 256, :]
        gate, up = _dot(b, wg, 1, 0), _dot(b, wu, 1, 0)
        gu_ref[0, at : at + 256, :] = gate
        gu_ref[1, at : at + 256, :] = up
        act_ref[at : at + 256, :] = (gate * jax.nn.sigmoid(gate) * up).astype(LOW)


def up_of(b, rest, ff):
    t, d = b.shape
    n, bf = rest.shape[0], 512
    per, third = d // bf, ff // d
    ins = [(b, (t, d), lambda j: (0, 0)),
           (rest, (n, d // n, bf), lambda j: (0, j // per, j % per)),
           (rest, (n, d // n, bf), lambda j: (0, third + j // per, j % per))]
    outs = [((2, t, ff), WIDE, (2, t, bf), lambda j: (0, 0, j)), ((t, ff), LOW, (t, bf), lambda j: (0, j))]
    return call(_up, "up", (ff // bf,), ins, outs, flops=4 * t * d * ff, trans=t * ff)


def _down(act_ref, h_ref, w_ref, y_ref):
    r = _dot(act_ref[...], flat(w_ref), 1, 0).astype(LOW)
    y_ref[...] = (h_ref[...].astype(WIDE) + r.astype(WIDE)).astype(LOW)


def down_of(act, h2, rest):
    t, ff = act.shape
    d, n, bt = h2.shape[1], rest.shape[0], 512
    row = lambda i: (i, 0)
    ins = [(act, (bt, ff), row), (h2, (bt, d), row), (rest, (n, ff // n, d), lambda i: (0, 2, 0))]
    return call(_down, "down", (t // bt,), ins, [((t, d), LOW, (bt, d), row)], flops=2 * t * d * ff)[0]


def _down_back(dy_ref, w_ref, gu_ref, dgu_ref, dw_ref, act_s):
    w = flat(w_ref)
    for at in range(0, dy_ref.shape[0], 256):
        here = slice(at, at + 256)
        da = _dot(dy_ref[here, :], w, 1, 1).astype(LOW).astype(WIDE)
        gate, up = gu_ref[0, here, :], gu_ref[1, here, :]
        s = jax.nn.sigmoid(gate)
        silu = gate * s
        act_s[here, :] = (silu * up).astype(LOW)
        dgu_ref[0, here, :] = (da * up * (s + silu * (1 - s))).astype(LOW)
        dgu_ref[1, here, :] = (da * silu).astype(LOW)
    dw_ref[...] = _dot(act_s[...].T, dy_ref[...], 1, 0).astype(LOW).reshape(dw_ref.shape)


def down_back(dy, rest, gu):
    t, d = dy.shape
    ff, n = gu.shape[2], rest.shape[0]
    rows = ff // n
    bf = 2 * rows
    ins = [(dy, (t, d), lambda j: (0, 0), 1), (rest, (2, rows, d), lambda j: (j, 2, 0)), (gu, (2, t, bf), lambda j: (0, 0, j))]
    outs = [((2, t, ff), LOW, (2, t, bf), lambda j: (0, 0, j)), (rest.shape, LOW, (2, rows, d), lambda j: (j, 2, 0))]
    return call(_down_back, "down_back", (ff // bf,), ins, outs, [pltpu.VMEM((t, bf), LOW)], flops=4 * t * d * ff, trans=t * ff)


def _dw(x_ref, g_ref, stack_ref, out_ref, xt_s):
    @pl.when(pl.program_id(0) == 0)
    def _():
        xt_s[...] = x_ref[...].T

    g = g_ref[...].reshape(g_ref.shape[-2:])
    out_ref[...] = _dot(xt_s[...], g, 1, 0).astype(LOW).reshape(out_ref.shape)


def dw_into(stack, at, x, g):
    t, d = x.shape
    parts, _, columns = g.shape
    n, per = stack.shape[0], columns // d
    ins = [(x, (t, d), lambda j: (0, 0), 1), (g, (1, t, d), lambda j: (j // per, 0, j % per)), (stack, None, None)]
    outs = [(stack.shape, LOW, (n, d // n, d), lambda j: (0, at + j, 0))]
    return call(_dw, "dw", (parts * per,), ins, outs, [pltpu.VMEM((d, t), LOW)], aliases={2: 0}, flops=2 * t * d * parts * columns)[0]


def norm_back(h, dn, dy):
    wide, dn = h.astype(WIDE), dn.astype(WIDE)
    s = rms(wide)
    back = s * dn - wide * (s * s * s * jnp.mean(dn * wide, -1, keepdims=True))
    return (dy.astype(WIDE) + back.astype(LOW).astype(WIDE)).astype(LOW)


def _up_back(dgu_ref, gu_ref, wo_ref, h_ref, dy_ref, dh_ref, do_ref):
    d = h_ref.shape[1]
    rows = wo_ref.shape[1]
    third = dgu_ref.shape[2] // d
    total = None
    for i in range(2 * third):
        w = gu_ref[:, i * rows : i * rows + rows, :].reshape(d, d)
        c = (i % third) * d
        part = _dot(dgu_ref[i // third, :, c : c + d], w, 1, 1)
        total = part if total is None else total + part
    dh = norm_back(h_ref[...], total.astype(LOW), dy_ref[...])
    dh_ref[...] = dh
    do_ref[...] = _dot(dh, flat(wo_ref), 1, 1).astype(LOW)


def up_back(dgu, rest, first, h2, dy):
    t, d = h2.shape
    ff, n, bt = dgu.shape[2], rest.shape[0], 256
    row = lambda i: (i, 0)
    ins = [(dgu, (2, bt, ff), lambda i: (0, i, 0)), (rest, (n, 2 * (ff // d) * (d // n), d), lambda i: (0, 0, 0), 1),
           (first, (n, d // n, d), lambda i: (0, 3, 0), 1), (h2, (bt, d), row), (dy, (bt, d), row)]
    return call(_up_back, "up_back", (t // bt,), ins, [((t, d), LOW, (bt, d), row)] * 2, flops=4 * t * d * ff + 2 * t * d * d)


def _attend_back(q_ref, k_ref, v_ref, o_ref, do_ref, lse_ref, cos_ref, sin_ref, dq_ref, dk_ref, dv_ref, dq_s, dk_s, dv_s, *, scale):
    bq, d = q_ref.shape[0], HEAD
    heads = q_ref.shape[1] // d
    iq = pl.program_id(1)
    e = scale * LOG2E

    @pl.when(iq == 0)
    def _():
        dk_s[...] = jnp.zeros_like(dk_s)
        dv_s[...] = jnp.zeros_like(dv_s)

    dq_s[...] = jnp.zeros_like(dq_s)
    cut = [slice(i * d, i * d + d) for i in range(heads)]
    lses = [lse_ref[0, i : i + 1, :] * LOG2E for i in range(heads)]
    deltas = [(do_ref[:, c].astype(WIDE) * o_ref[:, c].astype(WIDE)).T.sum(axis=0, keepdims=True) for c in cut]

    def block(start, keys, first, masked):
        here, mine = pl.ds(pl.multiple_of(start, keys), keys), slice(first, bq)
        scores = [_dot(k_ref[here, c], q_ref[mine, c], 1, 1) for c in cut]
        dps = [_dot(v_ref[here, c], do_ref[mine, c], 1, 1) for c in cut]
        ok = seen(keys, bq - first) if masked else None
        for i, c in enumerate(cut):
            p = jnp.exp2(scores[i] * e - lses[i][:, mine])
            if masked:
                p = jnp.where(ok, p, 0.0)
            ds = (p * (dps[i] - deltas[i][:, mine])).astype(LOW)
            dv_s[i, here, :] += _dot(p.astype(LOW), do_ref[mine, c], 1, 0)
            dk_s[i, here, :] += _dot(ds, q_ref[mine, c], 1, 0)
            dq_s[i, :, mine] += _dot(k_ref[here, c].T, ds, 1, 0)

    lax.fori_loop(0, iq, lambda j, _: block(j * bq, bq, 0, False), None)
    block(iq * bq, bq // 2, 0, True)
    block(iq * bq + bq // 2, bq // 2, bq // 2, True)
    mine = pl.ds(pl.multiple_of(iq * bq, bq), bq)
    for i, c in enumerate(cut):
        dq = (dq_s[i] * scale).T.astype(LOW).astype(WIDE)
        dq_ref[:, c] = turn(dq, cos_ref[mine, :], -sin_ref[mine, :]).astype(LOW)

    @pl.when(iq == pl.num_programs(1) - 1)
    def _():
        for i, c in enumerate(cut):
            dk = (dk_s[i] * scale).astype(LOW).astype(WIDE)
            dk_ref[:, c] = turn(dk, cos_ref[...], -sin_ref[...]).astype(LOW)
            dv_ref[:, c] = dv_s[i].astype(LOW)


def attend_back(qkv, o, do, lse, cos, sin):
    t, d = o.shape
    heads, bq = 4, 512
    wide = heads * HEAD
    per = d // wide
    mine = lambda h, i: (i, h)
    ins = [(qkv, (bq, wide), mine), (qkv, (t, wide), lambda h, i: (0, per + h)), (qkv, (t, wide), lambda h, i: (0, 2 * per + h)),
           (o, (bq, wide), mine), (do, (bq, wide), mine), (lse, (1, heads, bq), lambda h, i: (h, 0, i)),
           (cos, (t, HEAD), lambda h, i: (0, 0)), (sin, (t, HEAD), lambda h, i: (0, 0))]
    keys = lambda h, i: (0, h)
    outs = [((t, d), LOW, (bq, wide), mine), ((t, d), LOW, (t, wide), keys), ((t, d), LOW, (t, wide), keys)]
    scratch = [pltpu.VMEM((heads, HEAD, bq), WIDE), pltpu.VMEM((heads, t, HEAD), WIDE), pltpu.VMEM((heads, t, HEAD), WIDE)]
    return call(functools.partial(_attend_back, scale=HEAD**-0.5), "attend_back", (per, t // bq), ins, outs, scratch,
                flops=10 * t * t * d, trans=(d // HEAD) * t * t)


def _dw_first(a_ref, q_ref, k_ref, v_ref, o_ref, h_ref, out_ref, *, rows):
    n, _, d = out_ref.shape
    xt = a_ref[...].T
    for i, g_ref in enumerate((q_ref, k_ref, v_ref, h_ref)):
        if i == 3:
            xt = o_ref[...].T
        out_ref[:, i * rows : i * rows + rows, :] = _dot(xt, g_ref[...], 1, 0).astype(LOW).reshape(n, rows, d)


def dw_first(a, dq, dk, dv, o, dh2, n):
    t, d = a.shape
    bm = 256
    rows = -(-4 * d // n // 24) * 24
    whole = lambda i: (0, 0)
    part = lambda i: (0, i)
    ins = [(a, (t, bm), part)] + [(g, (t, d), whole, 1) for g in (dq, dk, dv)] + [(o, (t, bm), part), (dh2, (t, d), whole, 1)]
    outs = [((n, rows, d), LOW, (n * bm // d, rows, d), lambda i: (i, 0, 0))]
    body = functools.partial(_dw_first, rows=d // n)
    return call(body, "dw_first", (d // bm,), ins, outs, flops=8 * t * d * d)[0]


def _qkv_back(q_ref, k_ref, v_ref, w_ref, h_ref, dy_ref, dh_ref):
    d = h_ref.shape[1]
    rows = w_ref.shape[1] // 3
    total = None
    for i, g_ref in enumerate((q_ref, k_ref, v_ref)):
        part = _dot(g_ref[...], w_ref[:, i * rows : i * rows + rows, :].reshape(d, d), 1, 1)
        total = part if total is None else total + part
    dh_ref[...] = norm_back(h_ref[...], total.astype(LOW), dy_ref[...])


def qkv_back(dq, dk, dv, first, h, dy):
    t, d = h.shape
    n, bt = first.shape[0], 512
    row = lambda i: (i, 0)
    ins = [(g, (bt, d), row) for g in (dq, dk, dv)] + [(first, (n, 3 * d // n, d), lambda i: (0, 0, 0), 1), (h, (bt, d), row), (dy, (bt, d), row)]
    return call(_qkv_back, "qkv_back", (t // bt,), ins, [((t, d), LOW, (bt, d), row)], flops=6 * t * d * d)[0]


def _everyone(mine_ref, out_ref, held, send_sem, recv_sem, *, n):
    me = lax.axis_index("dp")
    barrier = pltpu.get_barrier_semaphore()
    for k in range(1, n):
        pl.semaphore_signal(barrier, inc=1, device_id={"dp": lax.rem(me + k, n)}, device_id_type=pl.DeviceIdType.MESH)
    pl.semaphore_wait(barrier, n - 1)
    copies = []
    for k in range(1, n):
        copies.append(pltpu.make_async_remote_copy(
            src_ref=mine_ref, dst_ref=held.at[me], send_sem=send_sem.at[k], recv_sem=recv_sem.at[k],
            device_id={"dp": lax.rem(me + k, n)}, device_id_type=pl.DeviceIdType.MESH))
        copies[-1].start()
    held[me] = mine_ref[...]
    for copy in copies:
        copy.wait()
    out_ref[...] = jnp.broadcast_to(jnp.sum(jnp.sum(held[...], 0), keepdims=True), out_ref.shape)


def everyone(part, n):
    vmem = pl.BlockSpec(memory_space=pltpu.VMEM)
    total = pl.pallas_call(
        functools.partial(_everyone, n=n), name="everyone", out_shape=jax.ShapeDtypeStruct(part.shape, WIDE), in_specs=[vmem], out_specs=vmem,
        scratch_shapes=[pltpu.VMEM((n, *part.shape), WIDE), pltpu.SemaphoreType.DMA((n,)), pltpu.SemaphoreType.DMA((n,))],
        compiler_params=pltpu.CompilerParams(collective_id=0, has_side_effects=True),
        cost_estimate=pl.CostEstimate(flops=1 << 20, transcendentals=0, bytes_accessed=2 * n * part.size * 4),
    )(part)
    return total[0, 0]


def adamw(w, m, v, g):
    m = 0.9 * m + 0.1 * g
    v = 0.95 * v + 0.05 * g * g
    step = m * lax.rsqrt(v + 1e-8) + 0.1 * w
    return (w - 0.02 * step).astype(LOW), m, v


def tables(t):
    half = HEAD // 2
    angle = jnp.arange(t, dtype=WIDE)[:, None] * THETA ** (-jnp.arange(half, dtype=WIDE) / half)
    cos, sin = jnp.cos(angle), jnp.sin(angle)
    return jnp.concatenate([cos, cos], 1), jnp.concatenate([-sin, sin], 1)


def solution(mesh):
    def gathered(stack):
        whole = lax.all_gather(stack, "dp", axis=0, tiled=True)
        return whole.reshape(-1, *stack.shape)

    def summed(stack, rows, before):
        if before:
            stack, before[-1] = lax.optimization_barrier((stack, before[-1]))
        before.append(lax.psum_scatter(stack.reshape(-1, stack.shape[2]), "dp", scatter_dimension=0, tiled=True)[:rows])

    def step(x, dy, *arrays):
        weights, m, v = (arrays[i : i + 7] for i in (0, 7, 14))
        layers, _, d = weights[0].shape
        axis_size = mesh.shape["dp"]
        ff = weights[4].shape[2]
        wq, wk, wv, wo, w_gate, w_up, w_down = weights
        split = lambda w: [w[:, i : i + d] for i in range(0, w.shape[1], d)]
        first, rest = [], []
        for n in range(layers):
            first.append(gathered(jnp.concatenate([wq[n], wk[n], wv[n], wo[n]], 0)))
            rest.append(gathered(jnp.concatenate([*split(w_gate[n]), *split(w_up[n]), w_down[n]], 0)))
        cos, sin = tables(x.shape[1])
        h, kept = x[0], []
        for n in range(layers):
            a, qkv = qkv_of(h, first[n], cos, sin)
            o, lse = attend(qkv)
            h2, b = out_of(o, h, first[n])
            gu, act = up_of(b, rest[n], ff)
            kept.append((h, a, qkv, o, lse, h2, b, gu))
            if n < layers - 1:
                h = down_of(act, h2, rest[n])
        by_h, sums = dy[0], []
        for n in reversed(range(layers)):
            h, a, qkv, o, lse, h2, b, gu = kept[n]
            dgu, stack = down_back(by_h, rest[n], gu)
            stack = dw_into(stack, 0, b, dgu)
            dgu, stack = lax.optimization_barrier((dgu, stack))
            summed(stack, rest[n].shape[1], sums)
            dh2, do = up_back(dgu, rest[n], first[n], h2, by_h)
            dq, dk, dv = attend_back(qkv, o, do, lse, cos, sin)
            stack = dw_first(a, dq, dk, dv, o, dh2, first[n].shape[0])
            if n > 0:
                dq, dk, dv, stack = lax.optimization_barrier((dq, dk, dv, stack))
                by_h = qkv_back(dq, dk, dv, first[n], h, dh2)
            summed(stack, first[n].shape[1], sums)
        squares = everyone(sum(jnp.sum(g.astype(WIDE).reshape(-1, 8, 128) ** 2, 0) for g in sums), axis_size)
        count = axis_size * sum(w.size for w in weights)
        factor = jnp.minimum(1.0, 0.5 * lax.rsqrt(squares / count + 1e-30))
        mine = [(sums[2 * i + 1], sums[2 * i]) for i in reversed(range(layers))]
        r = d // first[0].shape[0]
        wide = lambda g, at: jnp.concatenate([g[at + i * r : at + i * r + r] for i in range(ff // d)], 1)
        third = ff // d * r
        cuts = (lambda f, s: f[:r], lambda f, s: f[r : 2 * r], lambda f, s: f[2 * r : 3 * r], lambda f, s: f[3 * r :],
                lambda f, s: wide(s, 0), lambda f, s: wide(s, third), lambda f, s: s[2 * third :])
        gradients = [jnp.stack([cut(*mine[n]) for n in range(layers)]).astype(WIDE) * factor for cut in cuts]
        new = [adamw(w.astype(WIDE), m, v, g) for w, m, v, g in zip(weights, m, v, gradients, strict=True)]
        return tuple(one[which] for which in range(3) for one in new)

    states, cut = P(("rep", "dp"), None, None), P(None, "dp", None)
    return jax.shard_map(
        step,
        mesh=mesh,
        in_specs=(states, states) + (cut,) * 21,
        out_specs=(P("rep", "dp", None),) * 21,
        check_vma=False,
    )
```

```python
import functools

import jax
import jax.numpy as jnp
from jax import lax
from jax.experimental import pallas as pl
from jax.experimental.pallas import tpu as pltpu
from jax.sharding import PartitionSpec as P

NEG = -1e30
HIDDEN = 2 * NEG
LOG2E = 1.4426950408889634
VMEM = 50 * 2**20
HEAD = 128
THETA = 10000
NAMES = ("wq", "wk", "wv", "wo", "w_gate", "w_up", "w_down")
LOW, WIDE = jnp.bfloat16, jnp.float32


def _dot(a, b, ca, cb):
    return lax.dot_general(a, b, (((ca,), (cb,)), ((), ())), preferred_element_type=jnp.float32)


def call(body, name, grid, ins, outs, scratch=(), aliases=None, flops=0, trans=0, sem=None):
    specs = []
    for array, block, where, *buffers in ins:
        if block is None:
            specs.append(pl.BlockSpec(memory_space=pl.ANY))
        elif buffers:
            specs.append(pl.BlockSpec(block, where, pipeline_mode=pl.Buffered(buffers[0])))
        else:
            specs.append(pl.BlockSpec(block, where))
    out_specs = [pl.BlockSpec(block, where) for _, _, block, where in outs]
    shapes = [jax.ShapeDtypeStruct(shape, dtype) for shape, dtype, _, _ in outs]
    moved = sum(a.size * a.dtype.itemsize for a, *_ in ins) + sum(s.size * s.dtype.itemsize for s in shapes)
    return pl.pallas_call(
        body, name=name, grid=grid, in_specs=specs, out_specs=out_specs, out_shape=shapes, scratch_shapes=list(scratch),
        input_output_aliases=aliases or {},
        compiler_params=pltpu.CompilerParams(dimension_semantics=("arbitrary",) * len(grid), vmem_limit_bytes=VMEM),
        cost_estimate=pl.CostEstimate(flops=int(flops), transcendentals=int(trans), bytes_accessed=int(moved)),
    )(*(a for a, *_ in ins))


def flat(ref):
    w = ref[...]
    return w.reshape(w.shape[0] * w.shape[1], w.shape[2])


def rms(wide):
    return lax.rsqrt(jnp.mean(wide * wide, -1, keepdims=True) + 1e-6)


def turn(x, cos, sin):
    return x * cos + pltpu.roll(x, 64, 1) * sin


def _qkv(h_ref, wq_ref, wk_ref, wv_ref, cos_ref, sin_ref, a_ref, out_ref):
    d = h_ref.shape[1]
    wide = h_ref[...].astype(WIDE)
    a = (wide * rms(wide)).astype(LOW)
    a_ref[...] = a
    cos, sin = cos_ref[...], sin_ref[...]
    for n, w_ref in enumerate((wq_ref, wk_ref, wv_ref)):
        for at in range(0, d, 256):
            r = _dot(a, w_ref[:, :, at : at + 256].reshape(d, 256), 1, 0).astype(LOW)
            if n < 2:
                r = jnp.concatenate([turn(r[:, i : i + HEAD].astype(WIDE), cos, sin).astype(LOW) for i in (0, HEAD)], axis=1)
            out_ref[:, n * d + at : n * d + at + 256] = r


def qkv_of(h, first, cos, sin):
    t, d = h.shape
    n = first.shape[0]
    bt = 512
    rows = d // n
    ins = [(h, (bt, d), lambda i: (i, 0))]
    ins += [(first, (n, rows, d), lambda i, j=j: (0, j, 0)) for j in range(3)]
    ins += [(cos, (bt, HEAD), lambda i: (i, 0)), (sin, (bt, HEAD), lambda i: (i, 0))]
    outs = [((t, d), LOW, (bt, d), lambda i: (i, 0)), ((t, 3 * d), LOW, (bt, 3 * d), lambda i: (i, 0))]
    return call(_qkv, "qkv", (t // bt,), ins, outs, flops=6 * t * d * d)


def seen(keys, queries):
    return lax.broadcasted_iota(jnp.int32, (keys, queries), 1) >= lax.broadcasted_iota(jnp.int32, (keys, queries), 0)


def _attend(q_ref, k_ref, v_ref, o_ref, lse_ref, top_s, mix_s, *, scale):
    bq, d = q_ref.shape[0], HEAD
    heads = q_ref.shape[1] // d
    iq = pl.program_id(0)
    e = scale * LOG2E
    top_s[...] = jnp.full(top_s.shape, NEG, WIDE)
    mix_s[...] = jnp.zeros(mix_s.shape, WIDE)

    def block(start, keys, first, masked):
        here, mine = pl.ds(pl.multiple_of(start, keys), keys), slice(first, bq)
        ones = jnp.ones((8, keys), LOW)
        scores = [_dot(k_ref[here, i * d : i * d + d], q_ref[mine, i * d : i * d + d], 1, 1) for i in range(heads)]
        ok = seen(keys, bq - first) if masked else None
        weights, keeps = [], []
        for i, s in enumerate(scores):
            if masked:
                s = jnp.where(ok, s, HIDDEN)
            old = top_s[i : i + 1, mine]
            top = jnp.maximum(old, s.max(axis=0, keepdims=True))
            top_s[i : i + 1, mine] = top
            weights.append(jnp.exp2((s - top) * e).astype(LOW))
            keeps.append(jnp.exp2((old - top) * e))
        for i, (p, keep) in enumerate(zip(weights, keeps)):
            values = jnp.concatenate([v_ref[here, i * d : i * d + d].T, ones], axis=0)
            mix_s[i, :, mine] = mix_s[i, :, mine] * keep + _dot(values, p, 1, 0)

    lax.fori_loop(0, iq, lambda j, _: block(j * bq, bq, 0, False), None)
    block(iq * bq, bq // 2, 0, True)
    block(iq * bq + bq // 2, bq // 2, bq // 2, True)
    for i in range(heads):
        total = mix_s[i, d : d + 1, :]
        o_ref[:, i * d : i * d + d] = (mix_s[i, :d, :] * (1 / total)).T.astype(LOW)
        lse_ref[i // 4, i % 4 : i % 4 + 1, :] = top_s[i : i + 1, :] * scale + jnp.log(total)


def attend(qkv):
    t, d = qkv.shape[0], qkv.shape[1] // 3
    heads, bq = d // HEAD, 512
    ins = [(qkv, (bq, d), lambda i: (i, 0)), (qkv, (t, d), lambda i: (0, 1)), (qkv, (t, d), lambda i: (0, 2))]
    outs = [((t, d), LOW, (bq, d), lambda i: (i, 0)),
            ((heads // 4, 4, t), WIDE, (heads // 4, 4, bq), lambda i: (0, 0, i))]
    scratch = [pltpu.VMEM((heads, bq), WIDE), pltpu.VMEM((heads, HEAD + 8, bq), WIDE)]
    return call(functools.partial(_attend, scale=HEAD**-0.5), "attend", (t // bq,), ins, outs, scratch,
                flops=4 * t * t * d, trans=heads * t * t)


def _out(o_ref, h_ref, w_ref, h2_ref, b_ref):
    r = _dot(o_ref[...], flat(w_ref), 1, 0).astype(LOW)
    h2 = (h_ref[...].astype(WIDE) + r.astype(WIDE)).astype(LOW)
    h2_ref[...] = h2
    wide = h2.astype(WIDE)
    b_ref[...] = (wide * rms(wide)).astype(LOW)


def out_of(o, h, first):
    t, d = h.shape
    n, bt = first.shape[0], 512
    row = lambda i: (i, 0)
    ins = [(o, (bt, d), row), (h, (bt, d), row), (first, (n, d // n, d), lambda i: (0, 3, 0))]
    outs = [((t, d), LOW, (bt, d), row)] * 2
    return call(_out, "out", (t // bt,), ins, outs, flops=2 * t * d * d)


def _up(b_ref, g_ref, u_ref, gu_ref, act_ref):
    wg, wu = flat(g_ref), flat(u_ref)
    for at in range(0, b_ref.shape[0], 256):
        b = b_ref[at : at + 256, :]
        gate, up = _dot(b, wg, 1, 0), _dot(b, wu, 1, 0)
        gu_ref[0, at : at + 256, :] = gate
        gu_ref[1, at : at + 256, :] = up
        act_ref[at : at + 256, :] = (gate * jax.nn.sigmoid(gate) * up).astype(LOW)


def up_of(b, rest, ff):
    t, d = b.shape
    n, bf = rest.shape[0], 256
    per, third = d // bf, ff // d
    ins = [(b, (t, d), lambda j: (0, 0)),
           (rest, (n, d // n, bf), lambda j: (0, j // per, j % per)),
           (rest, (n, d // n, bf), lambda j: (0, third + j // per, j % per))]
    outs = [((2, t, ff), WIDE, (2, t, bf), lambda j: (0, 0, j)), ((t, ff), LOW, (t, bf), lambda j: (0, j))]
    return call(_up, "up", (ff // bf,), ins, outs, flops=4 * t * d * ff, trans=t * ff)


def _down(act_ref, h_ref, w_ref, y_ref):
    r = _dot(act_ref[...], flat(w_ref), 1, 0).astype(LOW)
    y_ref[...] = (h_ref[...].astype(WIDE) + r.astype(WIDE)).astype(LOW)


def down_of(act, h2, down):
    t, ff = act.shape
    down, place = down
    d, n, bt = h2.shape[1], down.shape[0], 512
    row = lambda i: (i, 0)
    ins = [(act, (bt, ff), row), (h2, (bt, d), row), (down, (n, ff // n, d), lambda i: (0, place, 0))]
    return call(_down, "down", (t // bt,), ins, [((t, d), LOW, (bt, d), row)], flops=2 * t * d * ff)[0]


def _down_back(dy_ref, w_ref, gu_ref, dgu_ref, dw_ref, act_s):
    w = flat(w_ref)
    for at in range(0, dy_ref.shape[0], 256):
        here = slice(at, at + 256)
        da = _dot(dy_ref[here, :], w, 1, 1).astype(LOW).astype(WIDE)
        gate, up = gu_ref[0, here, :], gu_ref[1, here, :]
        s = jax.nn.sigmoid(gate)
        silu = gate * s
        act_s[here, :] = (silu * up).astype(LOW)
        dgu_ref[0, here, :] = (da * up * (s + silu * (1 - s))).astype(LOW)
        dgu_ref[1, here, :] = (da * silu).astype(LOW)
    dw_ref[...] = _dot(act_s[...].T, dy_ref[...], 1, 0).astype(LOW).reshape(dw_ref.shape)


def down_back(dy, down, gu):
    t, d = dy.shape
    down, place = down
    ff, n = gu.shape[2], down.shape[0]
    rows = ff // n
    bf = 2 * rows
    ins = [(dy, (t, d), lambda j: (0, 0), 1), (down, (2, rows, d), lambda j: (j, place, 0)), (gu, (2, t, bf), lambda j: (0, 0, j))]
    outs = [((2, t, ff), LOW, (2, t, bf), lambda j: (0, 0, j)), ((n, 3 * rows, d), LOW, (2, rows, d), lambda j: (j, 2, 0))]
    return call(_down_back, "down_back", (ff // bf,), ins, outs, [pltpu.VMEM((t, bf), LOW)], flops=4 * t * d * ff, trans=t * ff)


def _dw(x_ref, g_ref, stack_ref, out_ref):
    g = g_ref[...].reshape(g_ref.shape[-2:])
    out_ref[...] = _dot(x_ref[...], g, 0, 0).astype(LOW).reshape(out_ref.shape)


def dw_into(stack, at, x, g):
    t, d = x.shape
    parts, _, columns = g.shape
    n, per = stack.shape[0], columns // d
    ins = [(x, (t, d), lambda j: (0, 0), 1), (g, (1, t, d), lambda j: (j // per, 0, j % per)), (stack, None, None)]
    outs = [(stack.shape, LOW, (n, d // n, d), lambda j: (0, at + j, 0))]
    return call(_dw, "dw", (parts * per,), ins, outs, aliases={2: 0}, flops=2 * t * d * parts * columns)[0]


def norm_back(h, dn, dy):
    wide, dn = h.astype(WIDE), dn.astype(WIDE)
    s = rms(wide)
    back = s * dn - wide * (s * s * s * jnp.mean(dn * wide, -1, keepdims=True))
    return (dy.astype(WIDE) + back.astype(LOW).astype(WIDE)).astype(LOW)


def _up_back(dgu_ref, gu_ref, wo_ref, h_ref, dy_ref, dh_ref, do_ref):
    d = h_ref.shape[1]
    rows = wo_ref.shape[1]
    third = dgu_ref.shape[2] // d
    total = None
    for i in range(2 * third):
        w = gu_ref[:, i * rows : i * rows + rows, :].reshape(d, d)
        c = (i % third) * d
        part = _dot(dgu_ref[i // third, :, c : c + d], w, 1, 1)
        total = part if total is None else total + part
    dh = norm_back(h_ref[...], total.astype(LOW), dy_ref[...])
    dh_ref[...] = dh
    do_ref[...] = _dot(dh, flat(wo_ref), 1, 1).astype(LOW)


def up_back(dgu, rest, first, h2, dy):
    t, d = h2.shape
    ff, n, bt = dgu.shape[2], rest.shape[0], 256
    row = lambda i: (i, 0)
    ins = [(dgu, (2, bt, ff), lambda i: (0, i, 0)), (rest, (n, 2 * (ff // d) * (d // n), d), lambda i: (0, 0, 0), 1),
           (first, (n, d // n, d), lambda i: (0, 3, 0), 1), (h2, (bt, d), row), (dy, (bt, d), row)]
    return call(_up_back, "up_back", (t // bt,), ins, [((t, d), LOW, (bt, d), row)] * 2, flops=4 * t * d * ff + 2 * t * d * d)


def _attend_back(q_ref, k_ref, v_ref, o_ref, do_ref, lse_ref, cos_ref, sin_ref, dq_ref, dk_ref, dv_ref, dq_s, dk_s, dv_s, *, scale):
    bq, d = q_ref.shape[0], HEAD
    heads = q_ref.shape[1] // d
    iq = pl.program_id(1)
    e = scale * LOG2E

    @pl.when(iq == 0)
    def _():
        dk_s[...] = jnp.zeros_like(dk_s)
        dv_s[...] = jnp.zeros_like(dv_s)

    dq_s[...] = jnp.zeros_like(dq_s)
    cut = [slice(i * d, i * d + d) for i in range(heads)]
    lses = [lse_ref[0, i : i + 1, :] * LOG2E for i in range(heads)]
    deltas = [(do_ref[:, c].astype(WIDE) * o_ref[:, c].astype(WIDE)).T.sum(axis=0, keepdims=True) for c in cut]

    def block(start, keys, first, masked):
        here, mine = pl.ds(pl.multiple_of(start, keys), keys), slice(first, bq)
        scores = [_dot(k_ref[here, c], q_ref[mine, c], 1, 1) for c in cut]
        dps = [_dot(v_ref[here, c], do_ref[mine, c], 1, 1) for c in cut]
        ok = seen(keys, bq - first) if masked else None
        for i, c in enumerate(cut):
            p = jnp.exp2(scores[i] * e - lses[i][:, mine])
            if masked:
                p = jnp.where(ok, p, 0.0)
            ds = (p * (dps[i] - deltas[i][:, mine])).astype(LOW)
            dv_s[i, here, :] += _dot(p.astype(LOW), do_ref[mine, c], 1, 0)
            dk_s[i, here, :] += _dot(ds, q_ref[mine, c], 1, 0)
            dq_s[i, :, mine] += _dot(k_ref[here, c].T, ds, 1, 0)

    lax.fori_loop(0, iq, lambda j, _: block(j * bq, bq, 0, False), None)
    block(iq * bq, bq // 2, 0, True)
    block(iq * bq + bq // 2, bq // 2, bq // 2, True)
    mine = pl.ds(pl.multiple_of(iq * bq, bq), bq)
    for i, c in enumerate(cut):
        dq = (dq_s[i] * scale).T.astype(LOW).astype(WIDE)
        dq_ref[:, c] = turn(dq, cos_ref[mine, :], -sin_ref[mine, :]).astype(LOW)

    @pl.when(iq == pl.num_programs(1) - 1)
    def _():
        for i, c in enumerate(cut):
            dk = (dk_s[i] * scale).astype(LOW).astype(WIDE)
            dk_ref[:, c] = turn(dk, cos_ref[...], -sin_ref[...]).astype(LOW)
            dv_ref[:, c] = dv_s[i].astype(LOW)


def attend_back(qkv, o, do, lse, cos, sin):
    t, d = o.shape
    heads, bq = 4, 512
    wide = heads * HEAD
    per = d // wide
    mine = lambda h, i: (i, h)
    ins = [(qkv, (bq, wide), mine), (qkv, (t, wide), lambda h, i: (0, per + h)), (qkv, (t, wide), lambda h, i: (0, 2 * per + h)),
           (o, (bq, wide), mine), (do, (bq, wide), mine), (lse, (1, heads, bq), lambda h, i: (h, 0, i)),
           (cos, (t, HEAD), lambda h, i: (0, 0)), (sin, (t, HEAD), lambda h, i: (0, 0))]
    keys = lambda h, i: (0, h)
    outs = [((t, d), LOW, (bq, wide), mine), ((t, d), LOW, (t, wide), keys), ((t, d), LOW, (t, wide), keys)]
    scratch = [pltpu.VMEM((heads, HEAD, bq), WIDE), pltpu.VMEM((heads, t, HEAD), WIDE), pltpu.VMEM((heads, t, HEAD), WIDE)]
    return call(functools.partial(_attend_back, scale=HEAD**-0.5), "attend_back", (per, t // bq), ins, outs, scratch,
                flops=10 * t * t * d, trans=(d // HEAD) * t * t)


def _dw_first(a_ref, q_ref, k_ref, v_ref, o_ref, h_ref, out_ref, *, rows):
    n, _, d = out_ref.shape
    xt = a_ref[...].T
    for i, g_ref in enumerate((q_ref, k_ref, v_ref, h_ref)):
        if i == 3:
            xt = o_ref[...].T
        out_ref[:, i * rows : i * rows + rows, :] = _dot(xt, g_ref[...], 1, 0).astype(LOW).reshape(n, rows, d)


def dw_first(a, dq, dk, dv, o, dh2, n):
    t, d = a.shape
    bm = 256
    rows = -(-4 * d // n // 24) * 24
    whole = lambda i: (0, 0)
    part = lambda i: (0, i)
    ins = [(a, (t, bm), part)] + [(g, (t, d), whole, 1) for g in (dq, dk, dv)] + [(o, (t, bm), part), (dh2, (t, d), whole, 1)]
    outs = [((n, rows, d), LOW, (n * bm // d, rows, d), lambda i: (i, 0, 0))]
    body = functools.partial(_dw_first, rows=d // n)
    return call(body, "dw_first", (d // bm,), ins, outs, flops=8 * t * d * d)[0]


def _qkv_back(q_ref, k_ref, v_ref, w_ref, h_ref, dy_ref, dh_ref):
    d = h_ref.shape[1]
    rows = w_ref.shape[1] // 3
    total = None
    for i, g_ref in enumerate((q_ref, k_ref, v_ref)):
        part = _dot(g_ref[...], w_ref[:, i * rows : i * rows + rows, :].reshape(d, d), 1, 1)
        total = part if total is None else total + part
    dh_ref[...] = norm_back(h_ref[...], total.astype(LOW), dy_ref[...])


def qkv_back(dq, dk, dv, first, h, dy):
    t, d = h.shape
    n, bt = first.shape[0], 512
    row = lambda i: (i, 0)
    ins = [(g, (bt, d), row) for g in (dq, dk, dv)] + [(first, (n, 3 * d // n, d), lambda i: (0, 0, 0), 1), (h, (bt, d), row), (dy, (bt, d), row)]
    return call(_qkv_back, "qkv_back", (t // bt,), ins, [((t, d), LOW, (bt, d), row)], flops=6 * t * d * d)[0]


def _everyone(mine_ref, out_ref, held, send_sem, recv_sem, *, n):
    me = lax.axis_index("dp")
    barrier = pltpu.get_barrier_semaphore()
    for k in range(1, n):
        pl.semaphore_signal(barrier, inc=1, device_id={"dp": lax.rem(me + k, n)}, device_id_type=pl.DeviceIdType.MESH)
    pl.semaphore_wait(barrier, n - 1)
    copies = []
    for k in range(1, n):
        copies.append(pltpu.make_async_remote_copy(
            src_ref=mine_ref, dst_ref=held.at[me], send_sem=send_sem.at[k], recv_sem=recv_sem.at[k],
            device_id={"dp": lax.rem(me + k, n)}, device_id_type=pl.DeviceIdType.MESH))
        copies[-1].start()
    held[me] = mine_ref[...]
    for copy in copies:
        copy.wait()
    out_ref[...] = jnp.broadcast_to(jnp.sum(jnp.sum(held[...], 0), keepdims=True), out_ref.shape)


def everyone(part, n):
    vmem = pl.BlockSpec(memory_space=pltpu.VMEM)
    total = pl.pallas_call(
        functools.partial(_everyone, n=n), name="everyone", out_shape=jax.ShapeDtypeStruct(part.shape, WIDE), in_specs=[vmem], out_specs=vmem,
        scratch_shapes=[pltpu.VMEM((n, *part.shape), WIDE), pltpu.SemaphoreType.DMA((n,)), pltpu.SemaphoreType.DMA((n,))],
        compiler_params=pltpu.CompilerParams(collective_id=0, has_side_effects=True),
        cost_estimate=pl.CostEstimate(flops=1 << 20, transcendentals=0, bytes_accessed=2 * n * part.size * 4),
    )(part)
    return total[0, 0]


def adamw(w, m, v, g):
    m = 0.9 * m + 0.1 * g
    v = 0.95 * v + 0.05 * g * g
    step = m * lax.rsqrt(v + 1e-8) + 0.1 * w
    return (w - 0.02 * step).astype(LOW), m, v


def tables(t):
    half = HEAD // 2
    angle = jnp.arange(t, dtype=WIDE)[:, None] * THETA ** (-jnp.arange(half, dtype=WIDE) / half)
    cos, sin = jnp.cos(angle), jnp.sin(angle)
    return jnp.concatenate([cos, cos], 1), jnp.concatenate([-sin, sin], 1)


def solution(mesh):
    def gathered(stack):
        whole = lax.all_gather(stack, "dp", axis=0, tiled=True)
        return whole.reshape(-1, *stack.shape)

    def summed(stack, rows, before):
        if before:
            stack, before[-1] = lax.optimization_barrier((stack, before[-1]))
        before.append(lax.psum_scatter(stack.reshape(-1, stack.shape[2]), "dp", scatter_dimension=0, tiled=True)[:rows])

    def step(x, dy, *arrays):
        weights, m, v = (arrays[i : i + 7] for i in (0, 7, 14))
        layers, _, d = weights[0].shape
        axis_size = mesh.shape["dp"]
        ff = weights[4].shape[2]
        wq, wk, wv, wo, w_gate, w_up, w_down = weights
        split = lambda w: [w[:, i : i + d] for i in range(0, w.shape[1], d)]
        first, rest, down = [], [], []
        for n in range(layers):
            first.append(gathered(jnp.concatenate([wq[n], wk[n], wv[n], wo[n]], 0)))
            halves = [*split(w_gate[n]), *split(w_up[n])]
            if n < layers - 1:
                rest.append(gathered(jnp.concatenate([*halves, w_down[n]], 0)))
                down.append((rest[n], 2))
            else:
                rest.append(gathered(jnp.concatenate(halves, 0)))
                down.append((gathered(w_down[n]), 0))
        cos, sin = tables(x.shape[1])
        h, kept = x[0], []
        for n in range(layers):
            a, qkv = qkv_of(h, first[n], cos, sin)
            o, lse = attend(qkv)
            h2, b = out_of(o, h, first[n])
            gu, act = up_of(b, rest[n], ff)
            kept.append((h, a, qkv, o, lse, h2, b, gu))
            if n < layers - 1:
                h = down_of(act, h2, down[n])
        by_h, sums = dy[0], []
        for n in reversed(range(layers)):
            h, a, qkv, o, lse, h2, b, gu = kept[n]
            dgu, stack = down_back(by_h, down[n], gu)
            stack = dw_into(stack, 0, b, dgu)
            dgu, stack = lax.optimization_barrier((dgu, stack))
            summed(stack, stack.shape[1], sums)
            dh2, do = up_back(dgu, rest[n], first[n], h2, by_h)
            dq, dk, dv = attend_back(qkv, o, do, lse, cos, sin)
            stack = dw_first(a, dq, dk, dv, o, dh2, first[n].shape[0])
            if n > 0:
                dq, dk, dv, stack = lax.optimization_barrier((dq, dk, dv, stack))
                by_h = qkv_back(dq, dk, dv, first[n], h, dh2)
            summed(stack, first[n].shape[1], sums)
        squares = everyone(sum(jnp.sum(g.astype(WIDE).reshape(-1, 8, 128) ** 2, 0) for g in sums), axis_size)
        count = axis_size * sum(w.size for w in weights)
        factor = jnp.minimum(1.0, 0.5 * lax.rsqrt(squares / count + 1e-30))
        mine = [(sums[2 * i + 1], sums[2 * i]) for i in reversed(range(layers))]
        r = d // first[0].shape[0]
        wide = lambda g, at: jnp.concatenate([g[at + i * r : at + i * r + r] for i in range(ff // d)], 1)
        third = ff // d * r
        cuts = (lambda f, s: f[:r], lambda f, s: f[r : 2 * r], lambda f, s: f[2 * r : 3 * r], lambda f, s: f[3 * r :],
                lambda f, s: wide(s, 0), lambda f, s: wide(s, third), lambda f, s: s[2 * third :])
        gradients = [jnp.stack([cut(*mine[n]) for n in range(layers)]).astype(WIDE) * factor for cut in cuts]
        new = [adamw(w.astype(WIDE), m, v, g) for w, m, v, g in zip(weights, m, v, gradients, strict=True)]
        return tuple(one[which] for which in range(3) for one in new)

    states, cut = P(("rep", "dp"), None, None), P(None, "dp", None)
    return jax.shard_map(
        step,
        mesh=mesh,
        in_specs=(states, states) + (cut,) * 21,
        out_specs=(P("rep", "dp", None),) * 21,
        check_vma=False,
    )
```
